8 devices in a mesh: fsdp: 8 (over z, y, x, core).
Axes of the slice: x: 2, y: 2, z: 1, core: 2. Of those that a mesh axis runs over, the one named last changes fastest.
Arguments:
- hidden: bfloat16 [16, 1024, 2048], P('fsdp')
- grad_out: bfloat16 [16, 1024, 2048], P('fsdp')
- positions: int32 [16, 1024], P('fsdp')
- gain_attn: bfloat16 [2048], P('fsdp')
- w_q: bfloat16 [2048, 2048], P('fsdp')
- b_q: bfloat16 [2048], P('fsdp')
- w_k: bfloat16 [2048, 2048], P('fsdp')
- b_k: bfloat16 [2048], P('fsdp')
- w_v: bfloat16 [2048, 2048], P('fsdp')
- b_v: bfloat16 [2048], P('fsdp')
- w_o: bfloat16 [2048, 2048], P('fsdp')
- gain_mlp: bfloat16 [2048], P('fsdp')
- w_gate: bfloat16 [2048, 5504], P('fsdp')
- w_up: bfloat16 [2048, 5504], P('fsdp')
- w_down: bfloat16 [5504, 2048], P('fsdp')
Outputs:
- output 1: bfloat16 [16, 1024, 2048], P('fsdp')
- output 2: bfloat16 [16, 1024, 2048], P('fsdp')
- output 3: float32 [2048], P('fsdp')
- output 4: float32 [2048, 2048], P('fsdp')
- output 5: float32 [2048], P('fsdp')
- output 6: float32 [2048, 2048], P('fsdp')
- output 7: float32 [2048], P('fsdp')
- output 8: float32 [2048, 2048], P('fsdp')
- output 9: float32 [2048], P('fsdp')
- output 10: float32 [2048, 2048], P('fsdp')
- output 11: float32 [2048], P('fsdp')
- output 12: float32 [2048, 5504], P('fsdp')
- output 13: float32 [2048, 5504], P('fsdp')
- output 14: float32 [5504, 2048], P('fsdp')
All inputs are finite; a program needn't handle non-finite values.
Results may differ from the reference program's by a relative error of at most 0.0189511.
Values are sent between devices in bfloat16 or wider.
A program may use at most 1 GiB of HBM per device.

```python
import math
import jax
import jax.numpy as jnp
from jax import lax

D = 2048
HEADS = 16
KV_HEADS = 16
HEAD = 128
FF = 5504
BATCH = 16
SEQ = 1024
NORM_EPS = 1e-6
ROPE_THETA = 1000000.0
GROUP_SEQS = math.gcd(BATCH, max(1, 512 // SEQ))


def setup_inputs(seed: int = 0) -> dict:
    key_list = jax.random.split(jax.random.key(seed), 16)
    q_width = HEADS * HEAD
    kv_width = KV_HEADS * HEAD
    scale_d = 1.0 / math.sqrt(D)

    def normal_f32(key_index, arr_shape):
        return jax.random.normal(key_list[key_index], arr_shape, jnp.float32)

    pos_gaps = jax.random.randint(key_list[2], (BATCH, SEQ), 1, 9)
    pos_starts = jax.random.randint(key_list[3], (BATCH, 1), 0, 512)
    positions = (pos_starts + jnp.cumsum(pos_gaps, axis=1) - 1).astype(jnp.int32)
    return {
        'hidden': normal_f32(0, (BATCH, SEQ, D)).astype(jnp.bfloat16),
        'grad_out': normal_f32(1, (BATCH, SEQ, D)).astype(jnp.bfloat16),
        'positions': positions,
        'gain_attn': (1.0 + 0.3 * normal_f32(4, (D,))).astype(jnp.bfloat16),
        'w_q': (normal_f32(5, (D, q_width)) * scale_d).astype(jnp.bfloat16),
        'b_q': (0.5 * normal_f32(6, (q_width,))).astype(jnp.bfloat16),
        'w_k': (normal_f32(7, (D, kv_width)) * scale_d).astype(jnp.bfloat16),
        'b_k': normal_f32(8, (kv_width,)).astype(jnp.bfloat16),
        'w_v': (normal_f32(9, (D, kv_width)) * scale_d).astype(jnp.bfloat16),
        'b_v': (0.5 * normal_f32(10, (kv_width,))).astype(jnp.bfloat16),
        'w_o': (normal_f32(11, (q_width, D)) / math.sqrt(q_width)).astype(jnp.bfloat16),
        'gain_mlp': (1.0 + 0.3 * normal_f32(12, (D,))).astype(jnp.bfloat16),
        'w_gate': (normal_f32(13, (D, FF)) * scale_d).astype(jnp.bfloat16),
        'w_up': (normal_f32(14, (D, FF)) * scale_d).astype(jnp.bfloat16),
        'w_down': (normal_f32(15, (FF, D)) / math.sqrt(FF)).astype(jnp.bfloat16),
    }


def rope_tables(positions):
    inv_freq = 1.0 / jnp.power(ROPE_THETA, jnp.arange(0, HEAD, 2).astype(jnp.float32) / HEAD)
    angles = positions.astype(jnp.float32)[:, :, None] * inv_freq
    angles = jnp.concatenate([angles, angles], axis=-1)[:, :, None, :]
    return jnp.cos(angles), jnp.sin(angles)


def rotate_half(vec_in):
    half_dim = vec_in.shape[-1] // 2
    return jnp.concatenate([-vec_in[..., half_dim:], vec_in[..., :half_dim]], axis=-1)


def rms_norm(val_f32, gain_vec):
    inv_rms = lax.rsqrt(jnp.mean(val_f32 * val_f32, axis=-1, keepdims=True) + NORM_EPS)
    return (val_f32 * inv_rms * gain_vec).astype(jnp.bfloat16).astype(jnp.float32)


def layer_forward(params, hidden, positions):
    gain_attn, w_q, b_q, w_k, b_k, w_v, b_v, w_o, gain_mlp, w_gate, w_up, w_down = params
    n_batch = hidden.shape[0]
    q_per_kv = HEADS // KV_HEADS
    cos_t, sin_t = rope_tables(positions)
    hidden_f32 = hidden.astype(jnp.float32)
    normed_attn = rms_norm(hidden_f32, gain_attn)
    q_lin = (jnp.einsum('bsd,de->bse', normed_attn, w_q) + b_q).reshape(n_batch, SEQ, HEADS, HEAD)
    k_lin = (jnp.einsum('bsd,de->bse', normed_attn, w_k) + b_k).reshape(n_batch, SEQ, KV_HEADS, HEAD)
    v_states = (jnp.einsum('bsd,de->bse', normed_attn, w_v) + b_v).astype(jnp.bfloat16).astype(jnp.float32)
    v_states = v_states.reshape(n_batch, SEQ, KV_HEADS, HEAD)
    q_states = (q_lin * cos_t + rotate_half(q_lin) * sin_t).astype(jnp.bfloat16).astype(jnp.float32)
    q_states = q_states.reshape(n_batch, SEQ, KV_HEADS, q_per_kv, HEAD)
    k_states = (k_lin * cos_t + rotate_half(k_lin) * sin_t).astype(jnp.bfloat16).astype(jnp.float32)
    scores = jnp.einsum('bqkgd,bskd->bkgqs', q_states, k_states) / math.sqrt(HEAD)
    causal = jnp.arange(SEQ)[:, None] >= jnp.arange(SEQ)[None, :]
    attn_probs = jax.nn.softmax(jnp.where(causal, scores, -1e30), axis=-1)
    attn_probs = attn_probs.astype(jnp.bfloat16).astype(jnp.float32)
    attn_out = jnp.einsum('bkgqs,bskd->bqkgd', attn_probs, v_states).astype(jnp.bfloat16).astype(jnp.float32)
    attn_out = attn_out.reshape(n_batch, SEQ, HEADS * HEAD)
    resid_mid = (hidden_f32 + jnp.einsum('bse,ed->bsd', attn_out, w_o)).astype(jnp.bfloat16).astype(jnp.float32)
    normed_mlp = rms_norm(resid_mid, gain_mlp)
    gate_pre = jnp.einsum('bsd,df->bsf', normed_mlp, w_gate)
    up_proj = jnp.einsum('bsd,df->bsf', normed_mlp, w_up)
    act_mlp = (jax.nn.silu(gate_pre) * up_proj).astype(jnp.bfloat16).astype(jnp.float32)
    return (resid_mid + jnp.einsum('bsf,fd->bsd', act_mlp, w_down)).astype(jnp.bfloat16)


def reference(hidden, grad_out, positions, gain_attn, w_q, b_q, w_k, b_k, w_v, b_v, w_o, gain_mlp, w_gate, w_up, w_down):
    params = tuple(weight_arr.astype(jnp.float32) for weight_arr in (gain_attn, w_q, b_q, w_k, b_k, w_v, b_v, w_o, gain_mlp, w_gate, w_up, w_down))
    n_steps = BATCH // GROUP_SEQS

    def scan_body(grad_acc, step_in):
        hid_step, gout_step, pos_step = step_in

        def forward_only(param_list, hid_in):
            return layer_forward(param_list, hid_in, pos_step)

        layer_out, pullback = jax.vjp(forward_only, params, hid_step)
        d_params, d_hidden = pullback(gout_step)
        return jax.tree.map(jnp.add, grad_acc, d_params), (layer_out, d_hidden)

    step_inputs = (
        hidden.reshape(n_steps, GROUP_SEQS, SEQ, D),
        grad_out.reshape(n_steps, GROUP_SEQS, SEQ, D),
        positions.reshape(n_steps, GROUP_SEQS, SEQ),
    )
    grad_init = jax.tree.map(jnp.zeros_like, params)
    grad_sum, (out_steps, dx_steps) = lax.scan(scan_body, grad_init, step_inputs)
    return (out_steps.reshape(BATCH, SEQ, D), dx_steps.reshape(BATCH, SEQ, D), grad_sum[0], grad_sum[1], grad_sum[2], grad_sum[3], grad_sum[4], grad_sum[5], grad_sum[6], grad_sum[7], grad_sum[8], grad_sum[9], grad_sum[10], grad_sum[11])
```

```python
import math
import jax
import jax.numpy as jnp
import numpy as np
from jax import lax
from jax.experimental import pallas as pl
from jax.experimental.pallas import tpu as pltpu
from jax.sharding import Mesh, PartitionSpec as P

HEAD_DIM = 128
NORM_EPS = 1e-6
ROPE_THETA = 1000000.0
BLOCK_Q = 256
SCALE = 1.0 / math.sqrt(HEAD_DIM)
ALL = ('chip', 'core')
BF16 = jnp.bfloat16
F32 = jnp.float32


def mm(lhs, rhs):
    return lax.dot_general(lhs, rhs, (((1,), (0,)), ((), ())), preferred_element_type=F32)


def mm_nt(lhs, rhs):
    return lax.dot_general(lhs, rhs, (((1,), (1,)), ((), ())), preferred_element_type=F32)


def mm_tn(lhs, rhs):
    return lax.dot_general(lhs, rhs, (((0,), (0,)), ((), ())), preferred_element_type=F32)


def rope_tables(positions):
    inv_freq = 1.0 / jnp.power(ROPE_THETA, jnp.arange(0, HEAD_DIM, 2).astype(F32) / HEAD_DIM)
    angles = positions.astype(F32)[:, :, None] * inv_freq
    cos_h, sin_h = jnp.cos(angles), jnp.sin(angles)
    return jnp.concatenate([cos_h, cos_h], axis=-1), jnp.concatenate([-sin_h, sin_h], axis=-1)


def swap_halves(vec):
    return pltpu.roll(vec, HEAD_DIM // 2, 1)


def softmax_rows(scores, row0):
    n_rows, n_keys = scores.shape
    row_id = row0 + lax.broadcasted_iota(jnp.int32, (n_rows, n_rows), 0)
    col_id = (n_keys - n_rows) + lax.broadcasted_iota(jnp.int32, (n_rows, n_rows), 1)
    diag = jnp.where(row_id >= col_id, scores[:, n_keys - n_rows:], -1e30)
    if n_keys > n_rows:
        scores = jnp.concatenate([scores[:, :n_keys - n_rows], diag], axis=1)
    else:
        scores = diag
    top = jnp.max(scores, axis=1, keepdims=True)
    expd = jnp.exp((scores - top) * SCALE)
    return expd * (1.0 / jnp.sum(expd, axis=1, keepdims=True))


def attn_fwd_kernel(qkv_ref, cos_ref, sin_ref, o_ref, rot_ref):
    cos_t, sin_t = cos_ref[0], sin_ref[0]
    for part in range(2):
        lin = qkv_ref[0, :, part * HEAD_DIM:(part + 1) * HEAD_DIM]
        rot_ref[0, :, part * HEAD_DIM:(part + 1) * HEAD_DIM] = (lin * cos_t + swap_halves(lin) * sin_t).astype(BF16)
    rot_ref[0, :, 2 * HEAD_DIM:] = qkv_ref[0, :, 2 * HEAD_DIM:].astype(BF16)
    n_seq = qkv_ref.shape[1]
    for row0 in range(0, n_seq, BLOCK_Q):
        n_keys = row0 + BLOCK_Q
        q_blk = rot_ref[0, row0:n_keys, :HEAD_DIM]
        k_blk = rot_ref[0, :n_keys, HEAD_DIM:2 * HEAD_DIM]
        v_blk = rot_ref[0, :n_keys, 2 * HEAD_DIM:]
        probs = softmax_rows(mm_nt(q_blk, k_blk), row0)
        o_ref[0, row0:n_keys, :] = mm(probs.astype(BF16), v_blk).astype(BF16)


def attn_bwd_kernel(rot_ref, do_ref, cos_ref, sin_ref, dqkv_ref, dbias_ref, dk_acc, dv_acc):
    n_seq = rot_ref.shape[1]
    cos_t, sin_t = cos_ref[0], sin_ref[0]
    dbias_q = jnp.zeros((1, HEAD_DIM), F32)
    for row0 in reversed(range(0, n_seq, BLOCK_Q)):
        n_keys = row0 + BLOCK_Q
        q_blk = rot_ref[0, row0:n_keys, :HEAD_DIM]
        k_blk = rot_ref[0, :n_keys, HEAD_DIM:2 * HEAD_DIM]
        v_blk = rot_ref[0, :n_keys, 2 * HEAD_DIM:]
        do_blk = do_ref[0, row0:n_keys, :]
        probs = softmax_rows(mm_nt(q_blk, k_blk), row0)
        d_probs = mm_nt(do_blk, v_blk)
        delta = jnp.sum(probs * d_probs, axis=1, keepdims=True)
        d_scores = (probs * (d_probs - delta) * SCALE).astype(BF16)
        dv_part = mm_tn(probs.astype(BF16), do_blk)
        dk_part = mm_tn(d_scores, q_blk)
        if n_keys == n_seq:
            dv_acc[...] = dv_part
            dk_acc[...] = dk_part
        else:
            dv_acc[:n_keys] += dv_part
            dk_acc[:n_keys] += dk_part
        dq_rot = mm(d_scores, k_blk).astype(BF16).astype(F32)
        dq_lin = dq_rot * cos_t[row0:n_keys] - swap_halves(dq_rot) * sin_t[row0:n_keys]
        dbias_q += jnp.sum(dq_lin, axis=0, keepdims=True)
        dqkv_ref[0, row0:n_keys, :HEAD_DIM] = dq_lin.astype(BF16)
    dk_rot = dk_acc[...].astype(BF16).astype(F32)
    dk_lin = dk_rot * cos_t - swap_halves(dk_rot) * sin_t
    dqkv_ref[0, :, HEAD_DIM:2 * HEAD_DIM] = dk_lin.astype(BF16)
    dv_lin = dv_acc[...].astype(BF16)
    dqkv_ref[0, :, 2 * HEAD_DIM:] = dv_lin
    dbias_ref[0, :, :HEAD_DIM] = dbias_q
    dbias_ref[0, :, HEAD_DIM:2 * HEAD_DIM] = jnp.sum(dk_lin, axis=0, keepdims=True)
    dbias_ref[0, :, 2 * HEAD_DIM:] = jnp.sum(dv_lin.astype(F32), axis=0, keepdims=True)


def head_spec(n_seq, width):
    return pl.BlockSpec((1, n_seq, width), lambda b, h: (b, 0, h))


def table_spec(n_seq):
    return pl.BlockSpec((1, n_seq, HEAD_DIM), lambda b, h: (b, 0, 0))


def attn_fwd(qkv_lin, cos_t, sin_t):
    n_batch, n_seq, width = qkv_lin.shape
    n_heads = width // (3 * HEAD_DIM)
    pairs = n_batch * n_heads * n_seq * (n_seq + BLOCK_Q) // 2
    return pl.pallas_call(
        attn_fwd_kernel,
        grid=(n_batch, n_heads),
        in_specs=[head_spec(n_seq, 3 * HEAD_DIM), table_spec(n_seq), table_spec(n_seq)],
        out_specs=[head_spec(n_seq, HEAD_DIM), head_spec(n_seq, 3 * HEAD_DIM)],
        out_shape=[jax.ShapeDtypeStruct((n_batch, n_seq, n_heads * HEAD_DIM), BF16), jax.ShapeDtypeStruct((n_batch, n_seq, width), BF16)],
        cost_estimate=pl.CostEstimate(flops=4 * pairs * HEAD_DIM * 2, bytes_accessed=qkv_lin.size * 6 + qkv_lin.size // 3 * 2, transcendentals=pairs),
        name='attn_fwd',
    )(qkv_lin, cos_t, sin_t)


def attn_bwd(rot, d_o, cos_t, sin_t):
    n_batch, n_seq, width = rot.shape
    n_heads = width // (3 * HEAD_DIM)
    pairs = n_batch * n_heads * n_seq * (n_seq + BLOCK_Q) // 2
    return pl.pallas_call(
        attn_bwd_kernel,
        grid=(n_batch, n_heads),
        in_specs=[head_spec(n_seq, 3 * HEAD_DIM), head_spec(n_seq, HEAD_DIM), table_spec(n_seq), table_spec(n_seq)],
        out_specs=[head_spec(n_seq, 3 * HEAD_DIM), pl.BlockSpec((1, 1, 3 * HEAD_DIM), lambda b, h: (b, 0, h))],
        out_shape=[jax.ShapeDtypeStruct((n_batch, n_seq, width), BF16), jax.ShapeDtypeStruct((n_batch, 1, width), F32)],
        scratch_shapes=[pltpu.VMEM((n_seq, HEAD_DIM), F32), pltpu.VMEM((n_seq, HEAD_DIM), F32)],
        cost_estimate=pl.CostEstimate(flops=10 * pairs * HEAD_DIM * 2, bytes_accessed=rot.size * 4 + rot.size // 3 * 2, transcendentals=pairs),
        name='attn_bwd',
    )(rot, d_o, cos_t, sin_t)


def norm_fwd(hidden, gain_vec):
    x_f32 = hidden.astype(F32)
    inv_rms = lax.rsqrt(jnp.mean(x_f32 * x_f32, axis=-1, keepdims=True) + NORM_EPS)
    return (x_f32 * inv_rms * gain_vec.astype(F32)).astype(BF16), inv_rms


def norm_bwd(hidden, inv_rms, gain_vec, d_normed):
    unit_rows = hidden.astype(F32) * inv_rms
    d_gain = jnp.sum(d_normed * unit_rows, axis=0)
    d_unit = d_normed * gain_vec.astype(F32)
    d_hidden = inv_rms * (d_unit - unit_rows * jnp.mean(d_unit * unit_rows, axis=-1, keepdims=True))
    return d_hidden, d_gain


def gather(shard):
    return lax.all_gather(shard, ALL, axis=0, tiled=True)


def to_partner(arr):
    return lax.ppermute(arr, 'core', [(0, 1), (1, 0)])


def after(arrs, *deps):
    n_arrs = len(arrs)
    return lax.optimization_barrier(tuple(arrs) + tuple(deps))[:n_arrs]


def split_kernel(core_ref, own_in, other_in, own_out, other_out):
    own_out[...] = own_in[...]
    other_out[...] = other_in[...]


def split_cols(core, arr, n_parts):
    n_rows, n_cols = arr.shape
    width = n_cols // n_parts
    rows = min(n_rows, 524288 // width)
    half = jax.ShapeDtypeStruct((n_rows, n_cols // 2), arr.dtype)
    out_spec = pl.BlockSpec((rows, width), lambda i, j, core_ref: (i, j))
    return pl.pallas_call(
        split_kernel,
        grid_spec=pltpu.PrefetchScalarGridSpec(
            num_scalar_prefetch=1, grid=(n_rows // rows, n_parts // 2),
            in_specs=[
                pl.BlockSpec((rows, width), lambda i, j, core_ref: (i, 2 * j + core_ref[0])),
                pl.BlockSpec((rows, width), lambda i, j, core_ref: (i, 2 * j + 1 - core_ref[0])),
            ],
            out_specs=[out_spec, out_spec],
        ),
        out_shape=[half, half],
        cost_estimate=pl.CostEstimate(flops=6 * arr.size, bytes_accessed=4 * arr.size, transcendentals=0), name='split_cols',
    )(core.reshape(1), arr, arr)


def scatter_rows(chip_sum):
    return lax.psum_scatter(chip_sum, 'chip', scatter_dimension=0, tiled=True)


def join_halves(core, rows):
    n_rows = rows.shape[0] // 2
    keep = jnp.where(core == 0, rows[:n_rows], rows[n_rows:])
    got = to_partner(jnp.where(core == 0, rows[n_rows:], rows[:n_rows]))
    return jnp.concatenate([jnp.where(core == 0, keep, got), jnp.where(core == 0, got, keep)], axis=1)


def by_head_kernel(q_ref, k_ref, v_ref, out_ref):
    for i in range(out_ref.shape[1] // HEAD_DIM):
        src = (q_ref, k_ref, v_ref)[i % 3]
        out_ref[:, i * HEAD_DIM:(i + 1) * HEAD_DIM] = src[:, i // 3 * HEAD_DIM:(i // 3 + 1) * HEAD_DIM]


def by_head(arrs):
    n_rows, n_cols = arrs[0].shape
    return pl.pallas_call(
        by_head_kernel, out_shape=jax.ShapeDtypeStruct((n_rows, 3 * n_cols), arrs[0].dtype),
        cost_estimate=pl.CostEstimate(flops=6 * arrs[0].size, bytes_accessed=12 * arrs[0].size, transcendentals=0), name='by_head',
    )(*arrs)


def from_heads_kernel(in_ref, *out_refs):
    for i in range(in_ref.shape[1] // HEAD_DIM):
        out_refs[i % 3][:, i // 3 * HEAD_DIM:(i // 3 + 1) * HEAD_DIM] = in_ref[:, i * HEAD_DIM:(i + 1) * HEAD_DIM]


def from_heads(arr):
    n_rows, n_cols = arr.shape
    block = 64
    return pl.pallas_call(
        from_heads_kernel, grid=(n_rows // block,),
        in_specs=[pl.BlockSpec((block, n_cols), lambda i: (i, 0))],
        out_specs=[pl.BlockSpec((block, n_cols // 3), lambda i: (i, 0))] * 3,
        out_shape=[jax.ShapeDtypeStruct((n_rows, n_cols // 3), arr.dtype)] * 3,
        cost_estimate=pl.CostEstimate(flops=2 * arr.size, bytes_accessed=8 * arr.size, transcendentals=0), name='from_heads',
    )(arr)


def by_head_vec(vecs):
    return jnp.concatenate([v.reshape(-1, 1, HEAD_DIM) for v in vecs], axis=1).reshape(-1)


def layer_step(hidden3, grad_out3, positions, gain_attn, w_q, b_q, w_k, b_k, w_v, b_v, w_o, gain_mlp, w_gate, w_up, w_down):
    core = lax.axis_index('core')
    n_batch, n_seq, width = hidden3.shape
    hidden = hidden3.reshape(n_batch * n_seq, width)
    grad_out = grad_out3.reshape(n_batch * n_seq, width)
    n_own = gain_attn.shape[0]
    vecs = lax.all_gather(jnp.concatenate([gain_attn, gain_mlp, by_head_vec([b_q, b_k, b_v])]), ALL, axis=0, tiled=False)
    gain_attn_f, gain_mlp_f, b_qkv = (vecs[:, lo:hi].reshape(-1) for lo, hi in ((0, n_own), (n_own, 2 * n_own), (2 * n_own, 5 * n_own)))
    w_qkv_f = gather(by_head([w_q, w_k, w_v]))
    w_o_f = gather(w_o)
    w_gate_f = gather(w_gate)
    w_up_f = gather(w_up)
    w_down_f = gather(w_down)

    gout_own, gout_other = split_cols(core, grad_out, 2)
    gout_got = to_partner(gout_other)
    cos_t, sin_t = rope_tables(positions)
    normed_attn, inv_attn = norm_fwd(hidden, gain_attn_f)
    na_own, na_other = split_cols(core, normed_attn, 8)
    na_got = to_partner(na_other)
    (normed_attn,) = after((normed_attn,), na_got, gout_got, cos_t, sin_t)
    qkv_lin = mm(normed_attn, w_qkv_f) + b_qkv.astype(F32)
    attn_out3, rot = attn_fwd(qkv_lin.reshape(n_batch, n_seq, -1), cos_t, sin_t)
    attn_out = attn_out3.reshape(n_batch * n_seq, width)
    ao_own, ao_other = split_cols(core, attn_out, 8)
    ao_got = to_partner(ao_other)
    resid_mid = (hidden.astype(F32) + mm(attn_out, w_o_f)).astype(BF16)
    normed_mlp, inv_mlp = norm_fwd(resid_mid, gain_mlp_f)
    nm_own, nm_other = split_cols(core, normed_mlp, 8)
    nm_got = to_partner(nm_other)
    (normed_mlp,) = after((normed_mlp,), nm_got, ao_got)
    gate_pre = mm(normed_mlp, w_gate_f)
    up_proj = mm(normed_mlp, w_up_f)
    act_mlp = (jax.nn.silu(gate_pre) * up_proj).astype(BF16)
    act_got = to_partner(act_mlp)

    sum_down = mm_tn(act_got, gout_got) + mm_tn(act_mlp, gout_own)
    rows_down = scatter_rows(sum_down)
    (grad_out_b,) = after((grad_out,), sum_down)
    d_act = mm_nt(grad_out_b, w_down_f).astype(BF16).astype(F32)
    gate_sig = jax.nn.sigmoid(gate_pre)
    d_gate = (d_act * up_proj * gate_sig * (1.0 + gate_pre * (1.0 - gate_sig))).astype(BF16)
    d_up = (d_act * gate_pre * gate_sig).astype(BF16)
    dg_got, du_got = to_partner(d_gate), to_partner(d_up)
    part_gate, part_up = mm_tn(nm_own, d_gate), mm_tn(nm_own, d_up)
    sum_gate = mm_tn(nm_got, dg_got) + part_gate
    sum_up = mm_tn(nm_got, du_got) + part_up
    d_w_gate, d_w_up = scatter_rows(sum_gate), scatter_rows(sum_up)
    d_gate, d_up = after((d_gate, d_up), sum_gate, sum_up)
    d_normed_mlp = (mm_nt(d_gate, w_gate_f) + mm_nt(d_up, w_up_f)).astype(BF16).astype(F32)
    d_resid_norm, d_gain_mlp = norm_bwd(resid_mid, inv_mlp, gain_mlp_f, d_normed_mlp)
    d_resid = (grad_out.astype(F32) + d_resid_norm).astype(BF16)
    dr_got = to_partner(d_resid)
    d_attn = mm_nt(d_resid, w_o_f).astype(BF16)
    sum_o = mm_tn(ao_got, dr_got) + mm_tn(ao_own, d_resid)
    d_w_o = scatter_rows(sum_o)
    (d_attn,) = after((d_attn,), sum_o)
    d_qkv3, d_bias = attn_bwd(rot, d_attn.reshape(n_batch, n_seq, width), cos_t, sin_t)
    d_qkv = d_qkv3.reshape(n_batch * n_seq, -1)
    dq_got = to_partner(d_qkv)
    sum_qkv = mm_tn(na_got, dq_got) + mm_tn(na_own, d_qkv)
    d_w_q, d_w_k, d_w_v = from_heads(scatter_rows(sum_qkv))
    d_qkv, act_mlp = after((d_qkv, act_mlp), sum_qkv)
    d_normed_attn = mm_nt(d_qkv, w_qkv_f).astype(BF16).astype(F32)
    d_hidden_norm, d_gain_attn = norm_bwd(hidden, inv_attn, gain_attn_f, d_normed_attn)
    grad_hidden = (d_resid.astype(F32) + d_hidden_norm).astype(BF16)
    layer_out = (resid_mid.astype(F32) + mm(act_mlp, w_down_f)).astype(BF16)
    d_w_down = join_halves(core, rows_down)

    d_vecs = jnp.stack([d_gain_attn, d_gain_mlp] + [jnp.sum(d_bias, axis=(0, 1)).reshape(-1, 3, HEAD_DIM)[:, j].reshape(-1) for j in range(3)])
    d_vecs = lax.all_gather(d_vecs, ALL, axis=0, tiled=False)
    me = lax.axis_index('chip') * 2 + core
    d_vecs = jnp.sum(lax.dynamic_slice_in_dim(d_vecs, me * n_own, n_own, axis=2), axis=0)
    return (
        layer_out.reshape(hidden3.shape), grad_hidden.reshape(hidden3.shape),
        d_vecs[0], d_w_q, d_vecs[2], d_w_k, d_vecs[3], d_w_v, d_vecs[4], d_w_o, d_vecs[1], d_w_gate, d_w_up, d_w_down,
    )


def solution(mesh):
    pair_mesh = Mesh(np.asarray(mesh.devices).reshape(-1, 2), ALL)
    act_spec, mat_spec, vec_spec = P(ALL, None, None), P(ALL, None), P(ALL)
    param_specs = (vec_spec, mat_spec, vec_spec, mat_spec, vec_spec, mat_spec, vec_spec, mat_spec, vec_spec, mat_spec, mat_spec, mat_spec)
    return jax.shard_map(
        layer_step, mesh=pair_mesh, in_specs=(act_spec, act_spec, mat_spec) + param_specs,
        out_specs=(act_spec, act_spec) + param_specs, check_vma=False,
    )
```
